128 devices in a mesh: rows: 32 (over z, x, core), width: 4 (over y).
Axes of the slice: x: 4, y: 4, z: 4, core: 2. Of those that a mesh axis runs over, the one named last changes fastest.
Arguments:
- weight_gate: float32 [2560, 9728], P('rows', 'width'), may hold values from -0.21875 to 0.21875
- moment_gate: float32 [2560, 9728], P('rows', 'width'), may hold values from -6 to 6
- square_gate: float32 [2560, 9728], P('rows', 'width'), may hold values from 0.1 to 10
- weight_up: float32 [2560, 9728], P('rows', 'width'), may hold values from -0.21875 to 0.21875
- moment_up: float32 [2560, 9728], P('rows', 'width'), may hold values from -6 to 6
- square_up: float32 [2560, 9728], P('rows', 'width'), may hold values from 0.1 to 10
- norm_gain: float32 [2560], P('rows'), may hold values from 0.25 to 1.75
Outputs:
- ready_gate: bfloat16 [2560, 9728], P(None, 'width')
- ready_up: bfloat16 [2560, 9728], P(None, 'width')
- column_gate: float32 [9728], P('width')
- column_up: float32 [9728], P('width')
The draws below stay inside these ranges and needn't reach their ends.
All inputs are finite; a program needn't handle non-finite values.
Results may differ from the reference program's by a relative error of at most 0.0004.
Values may be sent and summed in bfloat16 or wider, within the bound.
A program may use at most 128 MiB of HBM per device.

```python
import math
import jax
import jax.numpy as jnp
from jax import lax

D_MODEL = 2560
D_INNER = 9728


def with_spikes(values, rng, source, target, blocks, factor):
    def block_of(axis_at):
        return (jnp.arange(values.shape[axis_at]) // (values.shape[axis_at] // blocks)).reshape((-1,) + (1,) * (values.ndim - 1 - axis_at))

    one_side = jax.random.permutation(rng, blocks)[block_of(target)]
    second = (block_of(target) + blocks // 2) % blocks
    return jnp.where((block_of(source) == one_side) | (block_of(source) == second), factor * values, values)


def block_levels(rng, extent, pieces, smallest, top_value):
    loudness, own = 1.0, jax.random.fold_in(rng, 6)
    for dim, blocks in pieces:
        heights = jnp.exp(jax.random.uniform(jax.random.fold_in(own, dim), (blocks,), jnp.float32, smallest / len(pieces), top_value / len(pieces)))
        loudness = loudness * jnp.repeat(heights, extent[dim] // blocks).reshape([-1 if axis == dim else 1 for axis in range(len(extent))])
    return loudness


def normal_values(own_key, shape, scale, limit, split=(), held_as=jnp.bfloat16):
    array = scale * jax.random.normal(own_key, shape, jnp.float32)
    if split:
        array = array * block_levels(own_key, shape, split, -0.22, 0.18)
    return jnp.clip(array, -limit, limit).astype(held_as)


def noise_with(rng, dims, spread, most, shards, heavy, dtype=jnp.bfloat16):
    entries = spread * jax.random.normal(rng, dims, jnp.float32)
    if shards:
        entries = entries * block_levels(rng, dims, shards, -0.22, 0.18)
    return jnp.clip(with_spikes(entries, jax.random.fold_in(rng, 3), *heavy), -most, most).astype(dtype)


def setup_inputs(seed: int = 0) -> dict:
    arg_keys = jax.random.split(jax.random.key(seed), 8)
    return {
        "weight_gate": noise_with(arg_keys[0], (D_MODEL, D_INNER), D_MODEL ** -0.5, 0.21875, ((0, 32), (1, 4)), (0, 1, 32, 2.75), jnp.float32),
        "moment_gate": normal_values(arg_keys[1], (D_MODEL, D_INNER), 1.0, 6.0, ((0, 32), (1, 4)), jnp.float32),
        "square_gate": jnp.clip(jnp.exp(math.log(10.0) - 4.6051702 * jax.random.uniform(arg_keys[2], (D_MODEL, D_INNER), jnp.float32) ** block_levels(arg_keys[2], (D_MODEL, D_INNER), ((0, 32), (1, 4)), -0.2, 0.2)), 0.1, 10.0),
        "weight_up": noise_with(arg_keys[3], (D_MODEL, D_INNER), D_MODEL ** -0.5, 0.21875, ((0, 32), (1, 4)), (0, 1, 32, 2.75), jnp.float32),
        "moment_up": normal_values(arg_keys[4], (D_MODEL, D_INNER), 1.0, 6.0, ((0, 32), (1, 4)), jnp.float32),
        "square_up": jnp.clip(jnp.exp(math.log(10.0) - 4.6051702 * jax.random.uniform(arg_keys[5], (D_MODEL, D_INNER), jnp.float32) ** block_levels(arg_keys[5], (D_MODEL, D_INNER), ((0, 32), (1, 4)), -0.2, 0.2)), 0.1, 10.0),
        "norm_gain": jnp.clip(1.0 + 0.15 * jax.random.normal(arg_keys[6], (D_MODEL,), jnp.float32), 0.25, 1.75),
    }


learn_rate = 0.02
decay_rate = 0.1
tiny_value = 1e-08

def reference(weight_gate, moment_gate, square_gate, weight_up, moment_up, square_up, norm_gain):
    latest_gate = weight_gate - learn_rate * (moment_gate / (jnp.sqrt(square_gate) + tiny_value) + decay_rate * weight_gate)
    latest_up = weight_up - learn_rate * (moment_up / (jnp.sqrt(square_up) + tiny_value) + decay_rate * weight_up)
    latest_gained_gate = latest_gate * norm_gain[:, None]
    latest_gained_up = latest_up * norm_gain[:, None]
    column_gate = jnp.sqrt(lax.optimization_barrier(jnp.sum(latest_gained_gate * latest_gained_gate, axis=0)))
    ready_gate = (latest_gained_gate / column_gate).astype(jnp.bfloat16)
    column_up = jnp.sqrt(lax.optimization_barrier(jnp.sum(latest_gained_up * latest_gained_up, axis=0)))
    ready_up = (latest_gained_up / column_up).astype(jnp.bfloat16)
    return (ready_gate, ready_up, column_gate, column_up)
```

```python
import jax
import jax.numpy as jnp
from jax import lax
from jax.experimental import pallas as pl
from jax.experimental.pallas import tpu as pltpu
from jax.sharding import PartitionSpec as P

MESH = pl.DeviceIdType.MESH

learn_rate = 0.02
decay_rate = 0.1
tiny_value = 1e-08

SIDE = 4
ROWS = 80
WIDE = 2432
TILES = WIDE // 128
HALVES = ((0, 1280), (1280, 1152))
GATE, UP = 0, 1

ORDER = (
    ("first", 0, False, 0),
    ("first", 0, False, 1),
    ("then", 0, False, 0),
    ("first", 0, True, None),
    ("then", 0, False, 1),
    ("then", -1, False, 0),
    ("then", 1, False, 0),
    ("then", -1, False, 1),
    ("then", 1, False, 1),
    ("then", 0, True, None),
    ("then", 2, False, 0),
    ("then", 2, False, 1),
    ("then", -1, True, None),
    ("then", 1, True, None),
    ("then", 2, True, None),
)
STEPS = len(ORDER)
LAG = 2
LINKS = (("x", 1), ("z", 1), ("x", -1), ("z", -1))
FLIP = {0: 0, -1: 1, 1: 0, 2: 1}


def item_of(axis, s, step):
    which, other, forwarded, half = ORDER[step]
    array = (GATE if axis == "x" else UP) if which == "first" else (UP if axis == "x" else GATE)
    if half is None:
        flip = 0 if which == "first" else FLIP[other]
        half = flip if s == 1 else 1 - flip
    along = -s if forwarded else 0
    return array, ((other, along) if axis == "x" else (along, other)), half


def arrival_of(array, offset, half):
    for link, (axis, s) in enumerate(LINKS):
        for step in range(STEPS):
            a, (dz, dx), h = item_of(axis, s, step)
            dz, dx = (dz, dx - s) if axis == "x" else (dz - s, dx)
            if a == array and h == half and (dz - offset[0]) % SIDE == 0 and (dx - offset[1]) % SIDE == 0:
                return link, step
    raise ValueError("no arrival")


def gather_kernel(
    wg, mg, sg, wu, mu, su, gain,
    out_g, out_u, col,
    held, latest, part, peer, xsum, zsum,
    in_sem, red_send, red_recv, ici_send, ici_recv, d2d_send, d2d_recv,
):
    me = lax.axis_index("rows")
    core = lax.rem(me, 2)
    chip = me // 2
    x = lax.rem(chip, SIDE)
    z = chip // SIDE
    outs = (out_g, out_u)

    def at(dz, dx):
        return (lax.rem(z + dz + 2 * SIDE, SIDE) * SIDE + lax.rem(x + dx + 2 * SIDE, SIDE)) * 2 + core

    sibling = chip * 2 + 1 - core

    loads = []
    for i, ref in enumerate((wg, mg, sg, wu, mu, su)):
        load = pltpu.make_async_copy(ref, held.at[i], in_sem.at[i])
        load.start()
        loads.append(load)

    barrier = pltpu.get_barrier_semaphore()
    greeted = [sibling] + [at(0, d) for d in (1, 2, 3)] + [at(d, 0) for d in (1, 2, 3)]
    for device in greeted:
        pl.semaphore_signal(barrier, inc=1, device_id={"rows": device}, device_id_type=MESH)

    def remote(src, dst, send, recv, device):
        copy = pltpu.make_async_remote_copy(
            src_ref=src, dst_ref=dst, send_sem=send, recv_sem=recv,
            device_id={"rows": device}, device_id_type=MESH,
        )
        return copy

    line = jnp.broadcast_to(gain[...], (ROWS, ROWS))
    here = lax.broadcasted_iota(jnp.int32, (ROWS, ROWS), 0) == lax.broadcasted_iota(jnp.int32, (ROWS, ROWS), 1)
    rows_gain = jnp.sum(jnp.where(here, line, 0.0), axis=1, keepdims=True)

    for a in (GATE, UP):
        for load in loads[3 * a : 3 * a + 3]:
            load.wait()

        def adam(j, _, a=a):
            tile = pl.ds(pl.multiple_of(j * 128, 128), 128)
            w = held[3 * a, :, tile]
            value = w - learn_rate * (
                held[3 * a + 1, :, tile] / (jnp.sqrt(held[3 * a + 2, :, tile]) + tiny_value) + decay_rate * w
            )
            value = value * rows_gain
            latest[a, :, tile] = value
            part[a, :, tile] = jnp.sum(value * value, axis=0, keepdims=True)
            return 0

        lax.fori_loop(0, TILES, adam, 0)

    pl.semaphore_wait(barrier, len(greeted))

    copies = [remote(part.at[1 - core], peer, red_send.at[0], red_recv.at[0], sibling)]
    copies[0].start()
    copies[0].wait_recv()
    xsum[x] = part[core] + peer[...]
    for d in (1, 2, 3):
        copy = remote(xsum.at[x], xsum.at[x], red_send.at[d], red_recv.at[d], at(0, d))
        copy.start()
        copies.append(copy)
    for copy in copies[1:4]:
        copy.wait_recv()
    zsum[z] = xsum[0] + xsum[1] + xsum[2] + xsum[3]
    for d in (1, 2, 3):
        copy = remote(zsum.at[z], zsum.at[z], red_send.at[3 + d], red_recv.at[3 + d], at(d, 0))
        copy.start()
        copies.append(copy)
    for copy in copies[4:7]:
        copy.wait_recv()
    col[core] = jnp.sqrt(zsum[0] + zsum[1] + zsum[2] + zsum[3])
    copy = remote(col.at[core], col.at[core], red_send.at[7], red_recv.at[7], sibling)
    copy.start()
    copies.append(copy)
    copy.wait_recv()

    mine = pl.ds(pl.multiple_of(me * ROWS, 16), ROWS)
    for a in (GATE, UP):

        def scale(j, _, a=a):
            tile = pl.ds(pl.multiple_of(j * 128, 128), 128)
            inverse = 1.0 / col[a, :, tile]
            outs[a][mine, tile] = (latest[a, :, tile] * inverse).astype(jnp.bfloat16)
            return 0

        lax.fori_loop(0, TILES, scale, 0)

    def rows_of(offset):
        return pl.ds(pl.multiple_of(at(*offset) * ROWS, 16), ROWS)

    def piece(array, offset, half):
        return outs[array].at[rows_of(offset), pl.ds(*HALVES[half])]

    sent = [[None] * STEPS for _ in LINKS]
    arrived = set()
    passed = []

    def pass_on(src, slot):
        copy = remote(src, src, d2d_send.at[slot], d2d_recv.at[slot], sibling)
        copy.start()
        passed.append(copy)

    def arrive(link, step):
        if (link, step) in arrived:
            return
        arrived.add((link, step))
        axis, s = LINKS[link]
        array, (dz, dx), half = item_of(axis, s, step)
        offset = (dz, dx - s) if axis == "x" else (dz - s, dx)
        landed = piece(array, offset, half)
        pltpu.make_async_copy(landed, landed, ici_recv.at[link * STEPS + step]).wait()
        pass_on(landed, 2 + link * STEPS + step)

    for step in range(STEPS):
        for link, (axis, s) in enumerate(LINKS):
            array, offset, half = item_of(axis, s, step)
            if offset != (0, 0):
                arrive(*arrival_of(array, offset, half))
            src = piece(array, offset, half)
            slot = link * STEPS + step
            target = at(0, s) if axis == "x" else at(s, 0)
            copy = remote(src, src, ici_send.at[slot], ici_recv.at[slot], target)
            copy.start()
            sent[link][step] = copy
        if step == 0:
            for a in (GATE, UP):
                pass_on(outs[a].at[mine], a)
        if step >= LAG:
            for link in range(len(LINKS)):
                arrive(link, step - LAG)
    for step in range(STEPS - LAG, STEPS):
        for link in range(len(LINKS)):
            arrive(link, step)

    for copy in copies:
        copy.wait_send()
    for line_of in sent:
        for copy in line_of:
            copy.wait_send()
    for copy in passed:
        copy.wait_send()
    theirs = at(0, 0) + 1 - 2 * core
    for a in (GATE, UP):
        landed = outs[a].at[pl.ds(pl.multiple_of(theirs * ROWS, 16), ROWS)]
        pltpu.make_async_copy(landed, landed, d2d_recv.at[a]).wait()
    for link, (axis, s) in enumerate(LINKS):
        for step in range(STEPS):
            array, (dz, dx), half = item_of(axis, s, step)
            offset = (dz, dx - s) if axis == "x" else (dz - s, dx)
            row = at(*offset) + 1 - 2 * core
            landed = outs[array].at[pl.ds(pl.multiple_of(row * ROWS, 16), ROWS), pl.ds(*HALVES[half])]
            pltpu.make_async_copy(landed, landed, d2d_recv.at[2 + link * STEPS + step]).wait()


def gather(*args):
    hbm = pl.BlockSpec(memory_space=pltpu.HBM)
    vmem = pl.BlockSpec(memory_space=pltpu.VMEM)
    whole = SIDE * SIDE * 2 * ROWS
    return pl.pallas_call(
        gather_kernel,
        out_shape=(
            pltpu.VMEM((whole, WIDE), jnp.bfloat16),
            pltpu.VMEM((whole, WIDE), jnp.bfloat16),
            pltpu.VMEM((2, 1, WIDE), jnp.float32),
        ),
        in_specs=[hbm] * 6 + [vmem],
        out_specs=(vmem, vmem, vmem),
        scratch_shapes=[
            pltpu.VMEM((6, ROWS, WIDE), jnp.float32),
            pltpu.VMEM((2, ROWS, WIDE), jnp.float32),
            pltpu.VMEM((2, 1, WIDE), jnp.float32),
            pltpu.VMEM((1, WIDE), jnp.float32),
            pltpu.VMEM((SIDE, 1, WIDE), jnp.float32),
            pltpu.VMEM((SIDE, 1, WIDE), jnp.float32),
            pltpu.SemaphoreType.DMA((6,)),
            pltpu.SemaphoreType.DMA((8,)),
            pltpu.SemaphoreType.DMA((8,)),
            pltpu.SemaphoreType.DMA((4 * STEPS,)),
            pltpu.SemaphoreType.DMA((4 * STEPS,)),
            pltpu.SemaphoreType.DMA((2 + 4 * STEPS,)),
            pltpu.SemaphoreType.DMA((2 + 4 * STEPS,)),
        ],
        compiler_params=pltpu.CompilerParams(
            collective_id=0, has_side_effects=True, vmem_limit_bytes=36 * 2**20
        ),
        name="gather",
    )(*args)


PIECES = 8


def put_kernel(g, u, col, ready_g, ready_u, column_g, column_u, sem):
    copies = []
    for a, (src, dst) in enumerate(((g, ready_g), (u, ready_u))):
        rows = src.shape[0] // PIECES
        for i in range(PIECES):
            part = pl.ds(i * rows, rows)
            copy = pltpu.make_async_copy(src.at[part], dst.at[part], sem.at[a * PIECES + i])
            copy.start()
            copies.append(copy)
    column_g[...] = col[GATE, 0, :]
    column_u[...] = col[UP, 0, :]
    for copy in copies:
        copy.wait()


def put(g, u, col):
    hbm = pl.BlockSpec(memory_space=pl.ANY)
    vmem = pl.BlockSpec(memory_space=pltpu.VMEM)
    return pl.pallas_call(
        put_kernel,
        out_shape=(
            jax.ShapeDtypeStruct(g.shape, g.dtype),
            jax.ShapeDtypeStruct(u.shape, u.dtype),
            jax.ShapeDtypeStruct((WIDE,), jnp.float32),
            jax.ShapeDtypeStruct((WIDE,), jnp.float32),
        ),
        in_specs=[hbm, hbm, vmem],
        out_specs=(hbm, hbm, vmem, vmem),
        scratch_shapes=[pltpu.SemaphoreType.DMA((2 * PIECES,))],
        compiler_params=pltpu.CompilerParams(vmem_limit_bytes=2**20),
        name="put",
    )(g, u, col)


def per_device(weight_gate, moment_gate, square_gate, weight_up, moment_up, square_up, norm_gain):
    weights = (weight_gate, moment_gate, square_gate, weight_up, moment_up, square_up)
    weights = [pltpu.with_memory_space_constraint(a, pltpu.HBM) for a in weights]
    g, u, col = gather(*weights, norm_gain.reshape(1, ROWS))
    return put(g, u, col)


def solution(mesh):
    in_specs = (P("rows", "width"),) * 6 + (P("rows"),)
    out_specs = (P(None, "width"), P(None, "width"), P("width"), P("width"))
    return jax.shard_map(
        per_device, mesh=mesh, in_specs=in_specs, out_specs=out_specs, check_vma=False
    )
```
